256 devices in a mesh: code: 8 (over y, core), vocab: 32 (over x, z).
Axes of the slice: x: 4, y: 4, z: 8, core: 2. Of those that a mesh axis runs over, the one named last changes fastest.
Arguments:
- latent_activations: bfloat16 [512, 8192], P(None, 'vocab'), may hold values from -150 to 150
- code_fragments: bfloat16 [8, 21376, 8192], P('code', 'vocab'), may hold values from -0.25 to 0.25
- remaining_fragments: int32 [32, 6], P('vocab'), may hold values from 0 to 7, as said below
Outputs:
- log_probs: float32 [512, 128256], P('code', 'vocab')
The draws below stay inside these ranges and needn't reach their ends.
Inputs may be any that keep to these rules, and one draw needn't show every extreme that they name: `remaining_fragments`: each row holds 6 different share numbers in increasing order.
All inputs are finite; a program needn't handle non-finite values.
Results may differ from the reference program's by a relative error of at most 0.0003.
Values may be sent and summed in bfloat16 or wider, within the bound.
No kernel may reach another device: no remote copies, remote signals or barrier semaphores. Data moves between devices by JAX's collectives and lax.ppermute only.
A program may use at most 128 MiB of HBM per device.

```python
import jax
import jax.numpy as jnp
from jax import lax

D = 8192
ROWS = 668
BATCH = 512
SHARES = 8
DATA = 6
GROUPS = 32
VOCAB = 128256


def draw_latent_activations(key, part):
    first_key, second_key = jax.random.split(jax.random.fold_in(key, 11))
    standard = jax.random.truncated_normal(first_key, -5.0, 5.0, (BATCH, D), jnp.float32)
    row_scale = jnp.exp(jax.random.uniform(second_key, (BATCH, 1), jnp.float32, jnp.log(0.75), jnp.log(6.0)))
    return (standard * row_scale).astype(jnp.bfloat16)


def draw_remaining_fragments(key, part):
    scores = jax.random.randint(jax.random.fold_in(key, 5), (GROUPS, SHARES), 0, 1 << 20) * SHARES
    scores = scores + jnp.arange(SHARES, dtype=jnp.int32)[None, :]
    ordering = jnp.argsort(scores, axis=1, stable=True)
    return jnp.sort(ordering[:, :DATA], axis=1).astype(jnp.int32)


def shard_levels(stream_key, extent, shards, least, high):
    level, own = 1.0, jax.random.fold_in(stream_key, 6)
    for position, blocks in shards:
        draws = jnp.exp(jax.random.uniform(jax.random.fold_in(own, position), (blocks,), jnp.float32, least / len(shards), high / len(shards)))
        level = level * jnp.repeat(draws, extent[position] // blocks).reshape([-1 if axis == position else 1 for axis in range(len(extent))])
    return level


def noise(key, shape, spread, bound, pieces=(), held_as=jnp.bfloat16):
    drawn = jax.random.normal(key, shape, jnp.float32) * spread
    if len(pieces) > 0:
        drawn = shard_levels(key, shape, pieces, -0.22, 0.18) * drawn
    return jnp.clip(drawn, min=-bound, max=bound).astype(held_as)


def setup_inputs(seed: int = 0) -> dict:
    arg_keys = jax.random.split(jax.random.key(seed), 4)
    return {
        "latent_activations": draw_latent_activations(jax.random.fold_in(arg_keys[3], 71), 0),
        "code_fragments": noise(arg_keys[1], (SHARES, GROUPS * ROWS, D), (D // 16) ** -0.5, 0.25, ((0, 8), (1, 32))),
        "remaining_fragments": draw_remaining_fragments(jax.random.fold_in(arg_keys[3], 71), 0),
    }


def generator(count):
    nodes = jnp.cos(jnp.pi * (jnp.arange(count).astype(jnp.float32) + 0.5) / count)
    return jnp.concatenate([jnp.eye(count, dtype=jnp.float32), jnp.ones((1, count), jnp.float32), nodes[None, :]], axis=0)

def restoring_operator(chosen_row):
    select = (chosen_row[:, None] == jnp.arange(SHARES).astype(jnp.int32)[None, :]).astype(jnp.float32)
    square = jnp.dot(select, generator(DATA), precision=lax.Precision.HIGHEST)
    inverse = jnp.linalg.inv(square)
    return jnp.dot(inverse, select, precision=lax.Precision.HIGHEST)

def reference(latent_activations, code_fragments, remaining_fragments):
    blocks = code_fragments.reshape(SHARES, GROUPS, ROWS, D)

    def group_logits(fragment_position):
        block = blocks[:, fragment_position].reshape(SHARES * ROWS, D)
        encoded = jnp.dot(latent_activations.astype(jnp.float32), block.T.astype(jnp.float32), preferred_element_type=jnp.float32)
        encoded = encoded.reshape(BATCH, SHARES, ROWS)
        restored_lines = restoring_operator(remaining_fragments[fragment_position])
        payload_rows = jnp.einsum('js,bsr->bjr', restored_lines, encoded, precision=lax.Precision.HIGHEST)
        return payload_rows.reshape(BATCH, DATA * ROWS)
    logits = lax.map(group_logits, jnp.arange(GROUPS).astype(jnp.int32))
    logits = jnp.transpose(logits, (1, 0, 2)).reshape(BATCH, VOCAB)
    top = jnp.max(logits, axis=1, keepdims=True)
    total = jnp.sum(jnp.exp(logits - top), axis=1, keepdims=True)
    return logits - (top + jnp.log(total))
```

```python
import functools

import jax
import jax.numpy as jnp
import numpy as np
from jax import lax
from jax.experimental import pallas as pl
from jax.experimental.pallas import tpu as pltpu
from jax.sharding import PartitionSpec as P


X, Z, Y = 4, 8, 4
AXES = ("code", "vocab")
DATA = 6
SHARES = 8
WIDE = 768
MID, MID_EXP, STEP_EXP = 0, 1, 2

NODES = np.cos(np.float32(np.pi) * (np.arange(DATA, dtype=np.float32) + np.float32(0.5)) / np.float32(DATA)).astype(np.float32)


def pairs(move):
    out = []
    for y in range(Y):
        for core in range(2):
            for x in range(X):
                for z in range(Z):
                    to_x, to_z = move(x, z, core)
                    source = (y * 2 + core) * (X * Z) + x * Z + z
                    target = (y * 2 + core) * (X * Z) + (to_x % X) * Z + to_z % Z
                    out.append((source, target))
    return out


SWAP = [(code, code ^ 1) for code in range(2 * Y)]


def first(value, sign):
    return lax.ppermute(value, AXES, pairs(lambda x, z, c: (x + sign, z) if c == 0 else (x, z + sign)))


def first_core1(value, sign):
    return lax.ppermute(value, AXES, pairs(lambda x, z, c: (x, z) if c == 0 else (x, z + sign)))


def second(value, sign):
    return lax.ppermute(value, AXES, pairs(lambda x, z, c: (x, z + sign) if c == 0 else (x + sign, z)))


def second_core0(value, sign):
    return lax.ppermute(value, AXES, pairs(lambda x, z, c: (x, z + sign) if c == 0 else (x, z)))


def gather_pieces(own, core):
    def either(zero, one):
        return lax.select(jnp.broadcast_to(core == 0, zero.shape), zero, one)

    def two(a, b):
        return jnp.stack([a, b])

    s0 = own
    r1, r2 = first(s0, 1), first(s0, -1)
    r3 = first(r1, 1)
    r4 = first_core1(r2, -1)
    r5 = first_core1(r3, 1)
    r6 = first_core1(r4, -1)
    r7 = first_core1(r5, 1)
    c1, c2, d3, d4 = two(s0, r1), two(r2, r3), two(r4, r5), two(r6, r7)
    p1, p2 = second(c1, 1), second(c1, -1)
    p3, p4 = second(c2, 1), second(c2, -1)
    p5 = second(p1, 1)
    p6 = second(either(p2, d3), -1)
    p7 = second(p3, 1)
    p8 = second(either(p4, d4), -1)
    p9 = second(either(p5, d3), 1)
    p10 = second(p6, -1)
    p11 = second(either(p7, d4), 1)
    p12 = second(p8, -1)
    e1 = second_core0(p9, 1)
    e2 = second_core0(p12, -1)
    return [c1, c2, p1, p2, p3, p4, p5, p6, p7, p8, p9, p10, p11, p12, either(e1, d3), either(e2, d4)]


def piece_offsets():
    line = {"c1": (0, -1), "c2": (1, -2), "d3": (2, -3), "d4": (3, -4)}

    def along(core, name, other):
        return [(k, other) if core == 0 else (other, k) for k in line[name]]

    zero = [("c1", 0), ("c2", 0), ("c1", -1), ("c1", 1), ("c2", -1), ("c2", 1), ("c1", -2), ("c1", 2),
            ("c2", -2), ("c2", 2), ("c1", -3), ("c1", 3), ("c2", -3), ("c2", 3), ("c1", -4), ("c2", 4)]
    one = [("c1", 0), ("c2", 0), ("c1", -1), ("c1", 1), ("c2", -1), ("c2", 1), ("c1", -2), ("d3", 1),
           ("c2", -2), ("d4", 1), ("d3", -1), ("d3", 2), ("d4", -1), ("d4", 2), ("d3", 0), ("d4", 0)]
    return np.array([[along(core, *slot) for slot in slots] for core, slots in ((0, zero), (1, one))], np.int32)


def block_table(x, z, core):
    offsets = piece_offsets()
    index = ((offsets[..., 0] + x) % X) * Z + (offsets[..., 1] + z) % Z
    return jnp.where(core == 0, index, index[::-1]).astype(jnp.int32).reshape(-1)


def code_kernel(pieces, rows, table_ref, core_ref, *refs):
    mine, theirs = refs[:pieces], refs[pieces : 2 * pieces]
    w_hbm, out_ref, w_ref, acc_ref, sems = refs[2 * pieces :]
    half, depth = mine[0].shape[1], mine[0].shape[2]
    blocks = 2 * pieces

    def fetch(slot):
        block = table_ref[slot]
        columns = pl.ds(pl.multiple_of(block * depth, depth), depth)
        return pltpu.make_async_copy(w_hbm.at[:, columns], w_ref.at[:, columns], sems.at[slot])

    for slot in range(blocks):
        fetch(slot).start()

    def product(piece, base):
        total = None
        for k in range(2):
            columns = pl.ds(pl.multiple_of(table_ref[base + k] * depth, depth), depth)
            one = lax.dot_general(
                piece[k], w_ref[:, columns], (((1,), (1,)), ((), ())), preferred_element_type=jnp.float32
            )
            total = one if total is None else total + one
        return total

    for n in range(pieces):
        for k in range(2):
            fetch(2 * n + k).wait()
        value = product(mine[n], 2 * n)
        acc_ref[0] = value if n == 0 else acc_ref[0] + value
    for n in range(pieces):
        value = product(theirs[n], blocks + 2 * n)
        acc_ref[1] = value if n == 0 else acc_ref[1] + value

    core = core_ref[0]
    group = half // 4
    for part in range(2):
        for q in range(4):
            values = acc_ref[part, q * group : (q + 1) * group, :]
            high = jnp.max(values, axis=1, keepdims=True)
            low = jnp.min(values, axis=1, keepdims=True)
            packed = pack(values, low, high)
            at = jnp.where(core == part, 0, 4) + q
            out_ref[at] = packed


def pack(values, low, high):
    middle = 0.5 * low + 0.5 * high
    mid_exp = jnp.ceil(jnp.log2(jnp.maximum(jnp.abs(middle), 1e-30))) - 14.0
    mid = jnp.round(middle * jnp.exp2(-mid_exp))
    centre = mid * jnp.exp2(mid_exp)
    reach = jnp.maximum(jnp.maximum(high - centre, centre - low), 1e-25)
    step_exp = jnp.ceil((jnp.log2(reach) - 14.999) * 256.0)
    scaled = jnp.round((values - centre) * jnp.exp2(step_exp * (-1.0 / 256.0)))
    scaled = jnp.clip(scaled, -32767.0, 32767.0).astype(jnp.int32)
    rows, used = values.shape
    lane = lax.broadcasted_iota(jnp.int32, (rows, WIDE - used), 1)
    tail = jnp.where(
        lane == MID,
        mid.astype(jnp.int32),
        jnp.where(lane == MID_EXP, mid_exp.astype(jnp.int32), jnp.where(lane == STEP_EXP, step_exp.astype(jnp.int32), 0)),
    )
    return jnp.concatenate([scaled, tail], axis=1).astype(jnp.int16)


def decode_kernel(used, decode_ref, coded_ref, logits_ref, stats_ref):
    rows = coded_ref.shape[1]
    shares = []
    for s in range(SHARES):
        whole = coded_ref[s].astype(jnp.int32).astype(jnp.float32)
        mid, mid_exp, step_exp = (whole[:, used + k : used + k + 1] for k in (MID, MID_EXP, STEP_EXP))
        step = jnp.exp2(step_exp * (1.0 / 256.0))
        shares.append(whole[:, :used] * step + mid * jnp.exp2(mid_exp))
    lines = []
    for j in range(DATA):
        total = shares[0] * decode_ref[j, 0]
        for s in range(1, SHARES):
            total = total + shares[s] * decode_ref[j, s]
        lines.append(total)
    top = lines[0]
    for line in lines[1:]:
        top = jnp.maximum(top, line)
    top = jnp.max(top, axis=1, keepdims=True)
    total = jnp.exp(lines[0] - top)
    for line in lines[1:]:
        total = total + jnp.exp(line - top)
    total = jnp.sum(total, axis=1, keepdims=True)
    for j in range(DATA):
        logits_ref[:, j * used : (j + 1) * used] = lines[j]
    row = lax.broadcasted_iota(jnp.int32, (rows, 128), 0)
    lane = lax.broadcasted_iota(jnp.int32, (rows, 128), 1)
    both = jnp.where(lane == row, top, 0.0) + jnp.where(lane == row + rows, total, 0.0)
    stats_ref[...] = jnp.sum(both, axis=0, keepdims=True)


def finish_kernel(stats_ref, logits_ref, out_ref):
    rows = logits_ref.shape[0]
    stats = stats_ref[...]
    tops, totals = stats[:, :rows], stats[:, rows : 2 * rows]
    top = jnp.max(tops, axis=0, keepdims=True)
    total = jnp.sum(totals * jnp.exp(tops - top), axis=0, keepdims=True)
    normalizer = top + jnp.log(total)
    row = lax.broadcasted_iota(jnp.int32, (rows, rows), 0)
    lane = lax.broadcasted_iota(jnp.int32, (rows, rows), 1)
    column = jnp.sum(jnp.where(row == lane, normalizer, 0.0), axis=1, keepdims=True)
    out_ref[...] = logits_ref[...] - column


def decode_matrix(survivors):
    shares = jnp.arange(SHARES)
    alive = jnp.any(survivors[:, None] == shares[None, :], axis=0)
    nodes = jnp.asarray(NODES)
    here = alive[:DATA]
    lost = ~here
    ones, waves = alive[DATA], alive[DATA + 1]
    data = jnp.arange(DATA)
    other = jnp.sum(jnp.where(lost[None, :] & (data[None, :] != data[:, None]), nodes[None, :], 0.0), axis=1)
    two = ones & waves
    gap = jnp.where(two, nodes - other, jnp.where(waves, nodes, 1.0))
    from_ones = jnp.where(two, -other / gap, jnp.where(ones, 1.0, 0.0))
    from_waves = jnp.where(waves, 1.0 / gap, 0.0)
    padded = jnp.concatenate([nodes, jnp.zeros((SHARES - DATA,), jnp.float32)])
    known = alive & (shares < DATA)
    line_ones = jnp.where(shares == DATA, 1.0, jnp.where(known, -1.0, 0.0))
    line_waves = jnp.where(shares == DATA + 1, 1.0, jnp.where(known, -padded, 0.0))
    solved = from_ones[:, None] * line_ones[None, :] + from_waves[:, None] * line_waves[None, :]
    return jnp.where(here[:, None], (data[:, None] == shares[None, :]).astype(jnp.float32), solved)


def shards(latent_activations, code_fragments, remaining_fragments):
    weights = code_fragments[0]
    used, batch = weights.shape[0], latent_activations.shape[0]
    half = batch // 2
    code, vocab = lax.axis_index("code"), lax.axis_index("vocab")
    core, x, z = code % 2, vocab // Z, vocab % Z
    decode = decode_matrix(remaining_fragments[0])
    table = block_table(x, z, core)

    own = lax.dynamic_slice_in_dim(latent_activations, core * half, half, 0)
    mine = gather_pieces(own, core)
    theirs = [lax.ppermute(piece, "code", SWAP) for piece in mine]
    pieces = len(mine)

    smem, vmem, hbm = (pl.BlockSpec(memory_space=m) for m in (pltpu.SMEM, pltpu.VMEM, pl.ANY))
    coded = pl.pallas_call(
        functools.partial(code_kernel, pieces, batch),
        out_shape=jax.ShapeDtypeStruct((SHARES, batch // SHARES, WIDE), jnp.int16),
        in_specs=[smem, smem] + [vmem] * (2 * pieces) + [hbm],
        out_specs=vmem,
        scratch_shapes=[
            pltpu.VMEM(weights.shape, jnp.bfloat16),
            pltpu.VMEM((2, half, used), jnp.float32),
            pltpu.SemaphoreType.DMA((2 * pieces,)),
        ],
        compiler_params=pltpu.CompilerParams(vmem_limit_bytes=40 * 1024 * 1024),
        cost_estimate=pl.CostEstimate(flops=2 * batch * weights.size, bytes_accessed=2 * weights.size, transcendentals=0),
        name="code",
    )(table, core[None], *mine, *theirs, weights)
    exchanged = lax.all_to_all(coded, "code", split_axis=0, concat_axis=0, tiled=True)

    rows = batch // SHARES
    logits, stats = pl.pallas_call(
        functools.partial(decode_kernel, used),
        out_shape=(
            jax.ShapeDtypeStruct((rows, DATA * used), jnp.float32),
            jax.ShapeDtypeStruct((1, 2 * rows), jnp.float32),
        ),
        in_specs=[smem, vmem],
        out_specs=(vmem, vmem),
        name="decode",
    )(decode, exchanged)
    groups = lax.axis_size("vocab")
    spread = lax.all_to_all(jnp.broadcast_to(stats[None], (groups, 1, 2 * rows)), "vocab", 0, 0, tiled=True)
    return pl.pallas_call(
        finish_kernel,
        out_shape=jax.ShapeDtypeStruct((rows, DATA * used), jnp.float32),
        in_specs=[vmem, vmem],
        out_specs=vmem,
        name="finish",
    )(spread.reshape(groups, 2 * rows), logits)


def solution(mesh):
    return jax.shard_map(
        shards,
        mesh=mesh,
        in_specs=(P(None, "vocab"), P("code", "vocab", None), P("vocab", None)),
        out_specs=P("code", "vocab"),
        check_vma=False,
    )
```

```python
import functools

import jax
import jax.numpy as jnp
import numpy as np
from jax import lax
from jax.experimental import pallas as pl
from jax.experimental.pallas import tpu as pltpu
from jax.sharding import PartitionSpec as P


X, Z, Y = 4, 8, 4
AXES = ("code", "vocab")
DATA = 6
SHARES = 8
LANES = 128
FULL = 5
MID, MID_EXP, STEP_EXP = 0, 1, 2

NODES = np.cos(np.float32(np.pi) * (np.arange(DATA, dtype=np.float32) + np.float32(0.5)) / np.float32(DATA)).astype(np.float32)


def pairs(move):
    out = []
    for y in range(Y):
        for core in range(2):
            for x in range(X):
                for z in range(Z):
                    to_x, to_z = move(x, z, core)
                    source = (y * 2 + core) * (X * Z) + x * Z + z
                    target = (y * 2 + core) * (X * Z) + (to_x % X) * Z + to_z % Z
                    out.append((source, target))
    return out


SWAP = [(code, code ^ 1) for code in range(2 * Y)]


def first(value, sign):
    return lax.ppermute(value, AXES, pairs(lambda x, z, c: (x + sign, z) if c == 0 else (x, z + sign)))


def first_core1(value, sign):
    return lax.ppermute(value, AXES, pairs(lambda x, z, c: (x, z) if c == 0 else (x, z + sign)))


def second(value, sign):
    return lax.ppermute(value, AXES, pairs(lambda x, z, c: (x, z + sign) if c == 0 else (x + sign, z)))


def swap(value):
    return lax.ppermute(value, "code", SWAP)


def after(value, *others):
    return lax.optimization_barrier((value, *others))[0]


LINES = {"c": (0, -1, 1, -2), "d": (2, -3, 3, -4), "c0": (0, -1), "c1": (1, -2), "d0": (2, -3), "d1": (3, -4)}
STAGES = (
    ((("c", 0), ("c", -1), ("c", 1)), (("c", 0), ("c", -1), ("c", 1))),
    ((("c", -2), ("c", 2)), (("c", -2), ("d", 0))),
    ((("c", -3), ("c", 3)), (("d", -1), ("d", 1))),
    ((("c0", -4), ("c1", 4)), (("d0", -2), ("d1", 2))),
)


def block_table(x, z, core):
    offsets = np.array(
        [
            [(k, far) if own == 0 else (far, k) for stage in STAGES for name, far in stage[own] for k in LINES[name]]
            for own in range(2)
        ],
        np.int32,
    )
    both = np.concatenate([offsets.reshape(-1, 2), np.zeros((1, 2), np.int32)])
    turned = np.concatenate([offsets[::-1].reshape(-1, 2), np.zeros((1, 2), np.int32)])
    far_x, far_z = (jnp.where(core == 0, jnp.asarray(both[:, k]), jnp.asarray(turned[:, k])) for k in range(2))
    index = ((far_x + x) & (X - 1)) * Z + ((far_z + z) & (Z - 1))
    return jnp.where(jnp.arange(len(both)) == len(both) - 1, core, index).astype(jnp.int32)


def stage_kernel(start, pieces, opening, closing, table_ref, *refs):
    mine, theirs = refs[:pieces], refs[pieces : 2 * pieces]
    refs = refs[2 * pieces :]
    if opening:
        w_ref, out_ref = refs
        before_ref = acc_ref = out_ref
    elif closing:
        before_ref, w_ref, out_ref, acc_ref, line_ref = refs
    else:
        before_ref, w_ref, out_ref = refs
        acc_ref = out_ref
    each, half, depth = mine[0].shape
    total = w_ref.shape[1] // depth

    def weights(slot):
        return w_ref[:, pl.ds(pl.multiple_of(table_ref[slot] * depth, depth), depth)]

    for part, group in ((0, mine), (1, theirs)):
        for n, piece in enumerate(group):
            for k in range(0, each, 2):
                product = sum(
                    lax.dot_general(
                        weights(part * total + start + n * each + k + i),
                        piece[k + i],
                        (((1,), (1,)), ((), ())),
                        preferred_element_type=jnp.float32,
                    )
                    for i in range(2)
                )
                if k == 0 and n == 0:
                    acc_ref[part] = product if opening else before_ref[part] + product
                else:
                    acc_ref[part] += product
    if not closing:
        return
    core = table_ref[2 * total]
    for part in range(2):
        pack(acc_ref[part], line_ref)
        at = 4 * jnp.where(core == part, 0, 1)
        turned = line_ref[...].T.astype(jnp.int32).astype(jnp.int16)
        rows = half // 4
        for q in range(4):
            mine_rows = turned[q * rows : (q + 1) * rows]
            for k in range(FULL):
                out_ref[at + q, k * rows : (k + 1) * rows] = mine_rows[:, k * LANES : (k + 1) * LANES]
            rest = mine_rows[:, FULL * LANES : FULL * LANES + LANES // 4]
            tight = jnp.concatenate([rest[k * (rows // 4) : (k + 1) * (rows // 4)] for k in range(4)], axis=1)
            out_ref[at + q, FULL * rows :] = tight


def pack(values, line_ref):
    used, columns = values.shape
    high = jnp.max(values, axis=0, keepdims=True)
    low = jnp.min(values, axis=0, keepdims=True)
    middle = 0.5 * low + 0.5 * high
    mid_exp = jnp.ceil(jnp.log2(jnp.maximum(jnp.abs(middle), 1e-30))) - 14.0
    mid = jnp.round(middle * jnp.exp2(-mid_exp))
    centre = mid * jnp.exp2(mid_exp)
    reach = jnp.maximum(jnp.maximum(high - centre, centre - low), 1e-25)
    step_exp = jnp.ceil((jnp.log2(reach) - 14.999) * 256.0)
    scaled = jnp.round((values - centre) * jnp.exp2(step_exp * (-1.0 / 256.0)))
    line_ref[:used, :] = jnp.clip(scaled, -32767.0, 32767.0)
    row = lax.broadcasted_iota(jnp.int32, (4, columns), 0)
    line_ref[used : used + 4, :] = jnp.where(
        row == MID, mid, jnp.where(row == MID_EXP, mid_exp, jnp.where(row == STEP_EXP, step_exp, 0.0))
    )


def decode_kernel(used, decode_ref, coded_ref, logits_ref, stats_ref):
    rows = logits_ref.shape[0]
    shares = []
    for s in range(SHARES):
        flat = coded_ref[s].astype(jnp.int32).astype(jnp.float32)
        tight = flat[FULL * rows :]
        quarter = LANES // 4
        rest = jnp.concatenate([tight[:, k * quarter : (k + 1) * quarter] for k in range(4)], axis=0)
        whole = jnp.concatenate([flat[k * rows : (k + 1) * rows] for k in range(FULL)] + [rest], axis=1)
        mid, mid_exp, step_exp = (whole[:, used + k : used + k + 1] for k in (MID, MID_EXP, STEP_EXP))
        step = jnp.exp2(step_exp * (1.0 / 256.0))
        shares.append(whole[:, :used] * step + mid * jnp.exp2(mid_exp))
    lines = []
    for j in range(DATA):
        total = shares[0] * decode_ref[j, 0]
        for s in range(1, SHARES):
            total = total + shares[s] * decode_ref[j, s]
        lines.append(total)
    top = lines[0]
    for line in lines[1:]:
        top = jnp.maximum(top, line)
    top = jnp.max(top, axis=1, keepdims=True)
    total = jnp.exp(lines[0] - top)
    for line in lines[1:]:
        total = total + jnp.exp(line - top)
    total = jnp.sum(total, axis=1, keepdims=True)
    for j in range(DATA):
        logits_ref[:, j * used : (j + 1) * used] = lines[j]
    row = lax.broadcasted_iota(jnp.int32, (rows, 128), 0)
    lane = lax.broadcasted_iota(jnp.int32, (rows, 128), 1)
    both = jnp.where(lane == row, top, 0.0) + jnp.where(lane == row + rows, total, 0.0)
    line = jnp.sum(both, axis=0, keepdims=True)
    stats_ref[...] = jnp.broadcast_to(line[None], stats_ref.shape)


def finish_kernel(stats_ref, logits_ref, out_ref):
    rows = logits_ref.shape[0]
    stats = stats_ref[...]
    tops, totals = stats[:, :rows], stats[:, rows : 2 * rows]
    top = jnp.max(tops, axis=0, keepdims=True)
    total = jnp.sum(totals * jnp.exp(tops - top), axis=0, keepdims=True)
    normalizer = top + jnp.log(total)
    row = lax.broadcasted_iota(jnp.int32, (rows, rows), 0)
    lane = lax.broadcasted_iota(jnp.int32, (rows, rows), 1)
    column = jnp.sum(jnp.where(row == lane, normalizer, 0.0), axis=1, keepdims=True)
    out_ref[...] = logits_ref[...] - column


def decode_matrix(survivors):
    shares = jnp.arange(SHARES)
    alive = jnp.any(survivors[:, None] == shares[None, :], axis=0)
    nodes = jnp.asarray(NODES)
    here = alive[:DATA]
    lost = ~here
    ones, waves = alive[DATA], alive[DATA + 1]
    data = jnp.arange(DATA)
    other = jnp.sum(jnp.where(lost[None, :] & (data[None, :] != data[:, None]), nodes[None, :], 0.0), axis=1)
    two = ones & waves
    gap = jnp.where(two, nodes - other, jnp.where(waves, nodes, 1.0))
    from_ones = jnp.where(two, -other / gap, jnp.where(ones, 1.0, 0.0))
    from_waves = jnp.where(waves, 1.0 / gap, 0.0)
    padded = jnp.concatenate([nodes, jnp.zeros((SHARES - DATA,), jnp.float32)])
    known = alive & (shares < DATA)
    line_ones = jnp.where(shares == DATA, 1.0, jnp.where(known, -1.0, 0.0))
    line_waves = jnp.where(shares == DATA + 1, 1.0, jnp.where(known, -padded, 0.0))
    solved = from_ones[:, None] * line_ones[None, :] + from_waves[:, None] * line_waves[None, :]
    return jnp.where(here[:, None], (data[:, None] == shares[None, :]).astype(jnp.float32), solved)


def shards(latent_activations, code_fragments, remaining_fragments):
    weights = code_fragments[0]
    used, batch = weights.shape[0], latent_activations.shape[0]
    half = batch // 2
    code, vocab = lax.axis_index("code"), lax.axis_index("vocab")
    core, x, z = code % 2, vocab // Z, vocab % Z
    smem, vmem, hbm = (pl.BlockSpec(memory_space=m) for m in (pltpu.SMEM, pltpu.VMEM, pltpu.HBM))
    MB = 1024 * 1024

    def partial(stage, mine, theirs, before):
        opening, closing = stage == 0, stage == len(STAGES) - 1
        pieces, each = len(mine), mine[0].shape[0]
        blocks = 2 * pieces * each
        accumulator = (2, used, half)
        if closing:
            out = jax.ShapeDtypeStruct((SHARES, batch // SHARES * FULL + batch // SHARES // 4, LANES), jnp.int16)
        else:
            out = jax.ShapeDtypeStruct(accumulator, jnp.float32)
        scratch = []
        if closing:
            scratch = [pltpu.VMEM(accumulator, jnp.float32), pltpu.VMEM(((FULL + 1) * LANES, half), jnp.float32)]
        extra = [] if opening else [before]
        return pl.pallas_call(
            functools.partial(stage_kernel, 4 * (0, 3, 5, 7)[stage], pieces, opening, closing),
            out_shape=out,
            in_specs=[smem] + [vmem] * (2 * pieces + len(extra) + 1),
            out_specs=vmem,
            scratch_shapes=scratch,
            input_output_aliases={} if opening or closing else {1 + 2 * pieces: 0},
            compiler_params=pltpu.CompilerParams(vmem_limit_bytes=8 * MB),
            cost_estimate=pl.CostEstimate(
                flops=2 * blocks * half * depth * used, bytes_accessed=2 * blocks * depth * used, transcendentals=0
            ),
            name=f"stage{stage}",
        )(table, *mine, *theirs, *extra, weights)

    table = block_table(x, z, core)
    s0 = after(lax.dynamic_slice_in_dim(latent_activations, core * half, half, 0), table)
    depth = s0.shape[1]
    def either(zero, one):
        return lax.select(jnp.broadcast_to(core == 0, zero.shape), zero, one)

    r1, r2, r3 = first(s0, 1), first(s0, -1), first(s0, 2)
    c = jnp.stack([s0, r1, r2, r3])
    p1, p2 = second(c, 1), second(c, -1)
    r4, r5 = first_core1(r2, -1), first_core1(r3, 1)
    decode = decode_matrix(after(remaining_fragments[0], c))
    swapped = after(swap(c), r4, r5, decode)
    p3, p4 = second(after(p1, swapped), 1), second(after(p2, swapped), -1)
    r6, r7 = first_core1(r4, -1), first_core1(r5, 1)
    total = partial(0, [c, p1, p2], [swapped, swap(p1), swap(p2)], None)
    d = jnp.stack([r4, r5, r6, r7])
    p4 = either(p4, d)
    p5, p6 = second(after(either(p3, d), total), 1), second(after(p4, total), -1)
    total = partial(1, [p3, p4], [swap(p3), swap(p4)], total)
    p7, p8 = second(after(p5[:2], total), 1), second(after(p6[2:], total), -1)
    total = partial(2, [p5, p6], [swap(p5), swap(p6)], total)
    coded = partial(3, [p7, p8], [swap(p7), swap(p8)], total)
    exchanged = lax.all_to_all(coded, "code", split_axis=0, concat_axis=0, tiled=True)

    rows = batch // SHARES
    groups = lax.axis_size("vocab")
    logits, stats = pl.pallas_call(
        functools.partial(decode_kernel, used),
        out_shape=(
            jax.ShapeDtypeStruct((rows, DATA * used), jnp.float32),
            jax.ShapeDtypeStruct((groups, 1, 2 * rows), jnp.float32),
        ),
        in_specs=[smem, vmem],
        out_specs=(vmem, vmem),
        compiler_params=pltpu.CompilerParams(vmem_limit_bytes=16 * MB),
        name="decode",
    )(decode, exchanged)
    spread = lax.all_to_all(stats, "vocab", 0, 0, tiled=True)
    return pl.pallas_call(
        finish_kernel,
        out_shape=jax.ShapeDtypeStruct((rows, DATA * used), jnp.float32),
        in_specs=[vmem, vmem],
        out_specs=vmem,
        compiler_params=pltpu.CompilerParams(vmem_limit_bytes=16 * MB),
        name="finish",
    )(spread.reshape(groups, 2 * rows), logits)


def solution(mesh):
    return jax.shard_map(
        shards,
        mesh=mesh,
        in_specs=(P(None, "vocab"), P("code", "vocab", None), P("vocab", None)),
        out_specs=P("code", "vocab"),
        check_vma=False,
    )
```

```python
import functools

import jax
import jax.numpy as jnp
import numpy as np
from jax import lax
from jax.experimental import pallas as pl
from jax.experimental.pallas import tpu as pltpu
from jax.sharding import PartitionSpec as P


X, Z, Y = 4, 8, 4
AXES = ("code", "vocab")
DATA = 6
SHARES = 8
LANES = 128
FULL = 5
MID, MID_EXP, STEP_EXP = 0, 1, 2

NODES = np.cos(np.float32(np.pi) * (np.arange(DATA, dtype=np.float32) + np.float32(0.5)) / np.float32(DATA)).astype(np.float32)


def pairs(move):
    out = []
    for y in range(Y):
        for core in range(2):
            for x in range(X):
                for z in range(Z):
                    to_x, to_z = move(x, z, core)
                    source = (y * 2 + core) * (X * Z) + x * Z + z
                    target = (y * 2 + core) * (X * Z) + (to_x % X) * Z + to_z % Z
                    out.append((source, target))
    return out


SWAP = [(code, code ^ 1) for code in range(2 * Y)]


def first(value, sign):
    return lax.ppermute(value, AXES, pairs(lambda x, z, c: (x + sign, z) if c == 0 else (x, z + sign)))


def first_core1(value, sign):
    return lax.ppermute(value, AXES, pairs(lambda x, z, c: (x, z) if c == 0 else (x, z + sign)))


def second(value, sign):
    return lax.ppermute(value, AXES, pairs(lambda x, z, c: (x, z + sign) if c == 0 else (x + sign, z)))


def swap(value):
    return lax.ppermute(value, "code", SWAP)


def after(value, *others):
    return lax.optimization_barrier((value, *others))[0]


LINES = {"c": (0, -1, 1, -2), "d": (2, -3, 3, -4), "c0": (0, -1), "c1": (1, -2), "d0": (2, -3), "d1": (3, -4)}
STAGES = (
    ((("c", 0), ("c", -1), ("c", 1)), (("c", 0), ("c", -1), ("c", 1))),
    ((("c", -2), ("c", 2)), (("c", -2), ("d", 0))),
    ((("c", -3), ("c", 3)), (("d", -1), ("d", 1))),
    ((("c0", -4), ("c1", 4)), (("d0", -2), ("d1", 2))),
)


def block_table(x, z, core):
    offsets = np.array(
        [
            [(k, far) if own == 0 else (far, k) for stage in STAGES for name, far in stage[own] for k in LINES[name]]
            for own in range(2)
        ],
        np.int32,
    )
    both = np.concatenate([offsets.reshape(-1, 2), np.zeros((1, 2), np.int32)])
    turned = np.concatenate([offsets[::-1].reshape(-1, 2), np.zeros((1, 2), np.int32)])
    far_x, far_z = (jnp.where(core == 0, jnp.asarray(both[:, k]), jnp.asarray(turned[:, k])) for k in range(2))
    index = ((far_x + x) & (X - 1)) * Z + ((far_z + z) & (Z - 1))
    return jnp.where(jnp.arange(len(both)) == len(both) - 1, core, index).astype(jnp.int32)


def own_kernel(table_ref, hidden_ref, out_ref):
    half = out_ref.shape[0]
    core = table_ref[table_ref.shape[0] - 1]
    out_ref[...] = hidden_ref[pl.ds(pl.multiple_of(core * half, half), half), :]


def stage_kernel(start, pieces, opening, closing, table_ref, *refs):
    mine, theirs = refs[:pieces], refs[pieces : 2 * pieces]
    refs = refs[2 * pieces :]
    if opening:
        w_ref, out_ref = refs
        before_ref = acc_ref = out_ref
    elif closing:
        before_ref, w_ref, out_ref, acc_ref, line_ref = refs
    else:
        before_ref, w_ref, out_ref = refs
        acc_ref = out_ref
    each, half, depth = mine[0].shape
    total = w_ref.shape[1] // depth

    def weights(slot):
        return w_ref[:, pl.ds(pl.multiple_of(table_ref[slot] * depth, depth), depth)]

    for part, group in ((0, mine), (1, theirs)):
        for n, piece in enumerate(group):
            for k in range(0, each, 2):
                product = sum(
                    lax.dot_general(
                        weights(part * total + start + n * each + k + i),
                        piece[k + i],
                        (((1,), (1,)), ((), ())),
                        preferred_element_type=jnp.float32,
                    )
                    for i in range(2)
                )
                if k == 0 and n == 0:
                    acc_ref[part] = product if opening else before_ref[part] + product
                else:
                    acc_ref[part] += product
    if not closing:
        return
    core = table_ref[2 * total]
    for part in range(2):
        pack(acc_ref[part], line_ref)
        at = 4 * jnp.where(core == part, 0, 1)
        turned = line_ref[...].T.astype(jnp.int32).astype(jnp.int16)
        rows = half // 4
        for q in range(4):
            mine_rows = turned[q * rows : (q + 1) * rows]
            for k in range(FULL):
                out_ref[at + q, k * rows : (k + 1) * rows] = mine_rows[:, k * LANES : (k + 1) * LANES]
            rest = mine_rows[:, FULL * LANES : FULL * LANES + LANES // 4]
            tight = jnp.concatenate([rest[k * (rows // 4) : (k + 1) * (rows // 4)] for k in range(4)], axis=1)
            out_ref[at + q, FULL * rows :] = tight


def pack(values, line_ref):
    used, columns = values.shape
    high = jnp.max(values, axis=0, keepdims=True)
    low = jnp.min(values, axis=0, keepdims=True)
    middle = 0.5 * low + 0.5 * high
    mid_exp = jnp.ceil(jnp.log2(jnp.maximum(jnp.abs(middle), 1e-30))) - 14.0
    mid = jnp.round(middle * jnp.exp2(-mid_exp))
    centre = mid * jnp.exp2(mid_exp)
    reach = jnp.maximum(jnp.maximum(high - centre, centre - low), 1e-25)
    step_exp = jnp.ceil((jnp.log2(reach) - 14.999) * 256.0)
    scaled = jnp.round((values - centre) * jnp.exp2(step_exp * (-1.0 / 256.0)))
    line_ref[:used, :] = jnp.clip(scaled, -32767.0, 32767.0)
    row = lax.broadcasted_iota(jnp.int32, (4, columns), 0)
    line_ref[used : used + 4, :] = jnp.where(
        row == MID, mid, jnp.where(row == MID_EXP, mid_exp, jnp.where(row == STEP_EXP, step_exp, 0.0))
    )


def decode_matrix(survivors_ref):
    survivors = [survivors_ref[0, k] for k in range(DATA)]
    alive = [functools.reduce(jnp.logical_or, [one == s for one in survivors]) for s in range(SHARES)]
    lost = [jnp.logical_not(alive[j]) for j in range(DATA)]
    ones, waves = alive[DATA], alive[DATA + 1]
    two = jnp.logical_and(ones, waves)
    zero = jnp.float32(0.0)
    nodes = NODES.astype(np.float64)
    lines = []
    for j in range(DATA):
        others = [o for o in range(DATA) if o != j]
        both_ones = sum(jnp.where(lost[o], jnp.float32(-nodes[o] / (nodes[j] - nodes[o])), zero) for o in others)
        both_waves = sum(jnp.where(lost[o], jnp.float32(1.0 / (nodes[j] - nodes[o])), zero) for o in others)
        from_ones = jnp.where(two, both_ones, jnp.where(ones, jnp.float32(1.0), zero))
        from_waves = jnp.where(two, both_waves, jnp.where(waves, jnp.float32(1.0 / nodes[j]), zero))
        line = []
        for s in range(DATA):
            solved = jnp.where(alive[s], -(from_ones + from_waves * jnp.float32(nodes[s])), zero)
            line.append(jnp.where(alive[j], jnp.float32(s == j), solved))
        line.append(jnp.where(alive[j], zero, from_ones))
        line.append(jnp.where(alive[j], zero, from_waves))
        lines.append(line)
    return lines


def decode_kernel(used, survivors_ref, coded_ref, logits_ref, stats_ref):
    decode = decode_matrix(survivors_ref)
    rows = logits_ref.shape[0]
    shares = []
    for s in range(SHARES):
        flat = coded_ref[s].astype(jnp.int32).astype(jnp.float32)
        tight = flat[FULL * rows :]
        quarter = LANES // 4
        rest = jnp.concatenate([tight[:, k * quarter : (k + 1) * quarter] for k in range(4)], axis=0)
        whole = jnp.concatenate([flat[k * rows : (k + 1) * rows] for k in range(FULL)] + [rest], axis=1)
        mid, mid_exp, step_exp = (whole[:, used + k : used + k + 1] for k in (MID, MID_EXP, STEP_EXP))
        step = jnp.exp2(step_exp * (1.0 / 256.0))
        shares.append(whole[:, :used] * step + mid * jnp.exp2(mid_exp))
    lines = []
    for j in range(DATA):
        total = shares[0] * decode[j][0]
        for s in range(1, SHARES):
            total = total + shares[s] * decode[j][s]
        lines.append(total)
    top = lines[0]
    for line in lines[1:]:
        top = jnp.maximum(top, line)
    top = jnp.max(top, axis=1, keepdims=True)
    total = jnp.exp(lines[0] - top)
    for line in lines[1:]:
        total = total + jnp.exp(line - top)
    total = jnp.sum(total, axis=1, keepdims=True)
    for j in range(DATA):
        logits_ref[:, j * used : (j + 1) * used] = lines[j]
    row = lax.broadcasted_iota(jnp.int32, (rows, 128), 0)
    lane = lax.broadcasted_iota(jnp.int32, (rows, 128), 1)
    both = jnp.where(lane == row, top, 0.0) + jnp.where(lane == row + rows, total, 0.0)
    line = jnp.sum(both, axis=0, keepdims=True)
    stats_ref[...] = jnp.broadcast_to(line[None], stats_ref.shape)


def finish_kernel(stats_ref, logits_ref, out_ref):
    rows = logits_ref.shape[0]
    stats = stats_ref[...]
    tops, totals = stats[:, :rows], stats[:, rows : 2 * rows]
    top = jnp.max(tops, axis=0, keepdims=True)
    total = jnp.sum(totals * jnp.exp(tops - top), axis=0, keepdims=True)
    normalizer = top + jnp.log(total)
    row = lax.broadcasted_iota(jnp.int32, (rows, rows), 0)
    lane = lax.broadcasted_iota(jnp.int32, (rows, rows), 1)
    column = jnp.sum(jnp.where(row == lane, normalizer, 0.0), axis=1, keepdims=True)
    out_ref[...] = logits_ref[...] - column


def shards(latent_activations, code_fragments, remaining_fragments):
    weights = code_fragments[0]
    used, batch = weights.shape[0], latent_activations.shape[0]
    half = batch // 2
    code, vocab = lax.axis_index("code"), lax.axis_index("vocab")
    core, x, z = code % 2, vocab // Z, vocab % Z

    def partial(stage, mine, theirs, before):
        opening, closing = stage == 0, stage == len(STAGES) - 1
        pieces, each = len(mine), mine[0].shape[0]
        blocks = 2 * pieces * each
        accumulator = (2, used, half)
        if closing:
            out = jax.ShapeDtypeStruct((SHARES, batch // SHARES * FULL + batch // SHARES // 4, LANES), jnp.int16)
        else:
            out = jax.ShapeDtypeStruct(accumulator, jnp.float32)
        scratch = []
        if closing:
            scratch = [pltpu.VMEM(accumulator, jnp.float32), pltpu.VMEM(((FULL + 1) * LANES, half), jnp.float32)]
        extra = [] if opening else [before]
        return pl.pallas_call(
            functools.partial(stage_kernel, 4 * (0, 3, 5, 7)[stage], pieces, opening, closing),
            out_shape=out,
            in_specs=[smem] + [vmem] * (2 * pieces + len(extra) + 1),
            out_specs=vmem,
            scratch_shapes=scratch,
            input_output_aliases={} if opening or closing else {1 + 2 * pieces: 0},
            compiler_params=pltpu.CompilerParams(vmem_limit_bytes=8 * MB),
            cost_estimate=pl.CostEstimate(
                flops=2 * blocks * half * depth * used, bytes_accessed=2 * blocks * depth * used, transcendentals=0
            ),
        )(table, *mine, *theirs, *extra, weights)

    table = block_table(x, z, core)
    smem, vmem, _ = (pl.BlockSpec(memory_space=m) for m in (pltpu.SMEM, pltpu.VMEM, pltpu.HBM))
    MB = 1024 * 1024

    s0 = pl.pallas_call(
        own_kernel,
        out_shape=jax.ShapeDtypeStruct((half, latent_activations.shape[1]), latent_activations.dtype),
        in_specs=[smem, vmem],
        out_specs=vmem,
        compiler_params=pltpu.CompilerParams(vmem_limit_bytes=4 * MB),
        cost_estimate=pl.CostEstimate(flops=8 * batch * weights.size, bytes_accessed=2 * weights.size, transcendentals=0),
        name="own",
    )(table, latent_activations)
    depth = s0.shape[1]

    def either(zero, one):
        return lax.select(jnp.broadcast_to(core == 0, zero.shape), zero, one)

    r3, r1, r2 = first(s0, 2), first(s0, 1), first(s0, -1)
    c = jnp.stack([s0, r1, r2, r3])
    p1, p2 = second(c, 1), second(c, -1)
    r4, r5 = first_core1(r2, -1), first_core1(r3, 1)
    swapped = swap(c)
    p3, p4 = second(after(p1, swapped), 1), second(after(p2, swapped), -1)
    s1, s2 = swap(p1), swap(p2)
    r6, r7 = first_core1(r4, -1), first_core1(r5, 1)
    d = jnp.stack([r4, r5, r6, r7])
    p4 = either(p4, d)
    p5, p6 = second(either(p3, d), 1), second(p4, -1)
    total = partial(0, [c, p1, p2], [swapped, s1, s2], None)
    s3, s4 = swap(p3), swap(p4)
    total = partial(1, [p3, p4], [s3, s4], total)
    p7, p8 = second(p5[:2], 1), second(p6[2:], -1)
    total = partial(2, [p5, p6], [swap(p5), swap(p6)], total)
    coded = partial(3, [p7, p8], [swap(p7), swap(p8)], total)
    exchanged = lax.all_to_all(coded, "code", split_axis=0, concat_axis=0, tiled=True)

    rows = batch // SHARES
    groups = lax.axis_size("vocab")
    logits, stats = pl.pallas_call(
        functools.partial(decode_kernel, used),
        out_shape=(
            jax.ShapeDtypeStruct((rows, DATA * used), jnp.float32),
            jax.ShapeDtypeStruct((groups, 1, 2 * rows), jnp.float32),
        ),
        in_specs=[smem, vmem],
        out_specs=(vmem, vmem),
        compiler_params=pltpu.CompilerParams(vmem_limit_bytes=16 * MB),
        name="decode",
    )(remaining_fragments, exchanged)
    spread = lax.all_to_all(stats, "vocab", 0, 0, tiled=True)
    return pl.pallas_call(
        finish_kernel,
        out_shape=jax.ShapeDtypeStruct((rows, DATA * used), jnp.float32),
        in_specs=[vmem, vmem],
        out_specs=vmem,
        compiler_params=pltpu.CompilerParams(vmem_limit_bytes=16 * MB),
        name="finish",
    )(spread.reshape(groups, 2 * rows), logits)


def solution(mesh):
    return jax.shard_map(
        shards,
        mesh=mesh,
        in_specs=(P(None, "vocab"), P("code", "vocab", None), P("vocab", None)),
        out_specs=P("code", "vocab"),
        check_vma=False,
    )
```
